8 devices in a mesh: fsdp: 2 (over z, y), tp: 4 (over x, core).
Axes of the slice: x: 2, y: 2, z: 1, core: 2. Of those that a mesh axis runs over, the one named last changes fastest.
Arguments:
- x_in: bfloat16 [256, 256, 1024], P('fsdp')
- seq_lens: int32 [256], P('fsdp')
- grad_out: bfloat16 [256, 256, 1024], P('fsdp')
- ln1_gain: bfloat16 [1024], P('fsdp')
- ln1_bias: bfloat16 [1024], P('fsdp')
- w_query: bfloat16 [1024, 16, 64], P('fsdp', 'tp')
- b_query: bfloat16 [1024], P(('tp', 'fsdp'))
- w_key: bfloat16 [1024, 16, 64], P('fsdp', 'tp')
- b_key: bfloat16 [1024], P(('tp', 'fsdp'))
- w_value: bfloat16 [1024, 16, 64], P('fsdp', 'tp')
- b_value: bfloat16 [1024], P(('tp', 'fsdp'))
- w_out: bfloat16 [16, 64, 1024], P('tp', None, 'fsdp')
- b_out: bfloat16 [1024], P('fsdp')
- ln2_gain: bfloat16 [1024], P('fsdp')
- ln2_bias: bfloat16 [1024], P('fsdp')
- w_fc1: bfloat16 [1024, 4096], P('fsdp', 'tp')
- b_fc1: bfloat16 [4096], P(('tp', 'fsdp'))
- w_fc2: bfloat16 [4096, 1024], P('tp', 'fsdp')
- b_fc2: bfloat16 [1024], P('fsdp')
Outputs:
- output 1: bfloat16 [256, 256, 1024], P('fsdp')
- output 2: bfloat16 [256, 256, 1024], P('fsdp')
- output 3: float32 [1024], P('fsdp')
- output 4: float32 [1024], P('fsdp')
- output 5: float32 [1024, 16, 64], P('fsdp', 'tp')
- output 6: float32 [1024], P(('tp', 'fsdp'))
- output 7: float32 [1024, 16, 64], P('fsdp', 'tp')
- output 8: float32 [1024], P(('tp', 'fsdp'))
- output 9: float32 [1024, 16, 64], P('fsdp', 'tp')
- output 10: float32 [1024], P(('tp', 'fsdp'))
- output 11: float32 [16, 64, 1024], P('tp', None, 'fsdp')
- output 12: float32 [1024], P('fsdp')
- output 13: float32 [1024], P('fsdp')
- output 14: float32 [1024], P('fsdp')
- output 15: float32 [1024, 4096], P('fsdp', 'tp')
- output 16: float32 [4096], P(('tp', 'fsdp'))
- output 17: float32 [4096, 1024], P('tp', 'fsdp')
- output 18: float32 [1024], P('fsdp')
All inputs are finite; a program needn't handle non-finite values.
Results may differ from the reference program's by a relative error of at most 0.0164221.
Values are sent between devices in bfloat16 or wider.
A program may use at most 1.25 GiB of HBM per device.

```python
import jax
import jax.numpy as jnp
from jax import lax

D = 1024
HEADS = 16
HEAD = 64
FF = 4096
BATCH = 256
SEQ = 256
LN_EPS = 1e-5
ROPE_BASE = 10000.0


def draw_normal(rand_key, shape_dims, spread):
    return jax.random.normal(rand_key, shape_dims, jnp.float32) * spread


def setup_inputs(seed: int = 0) -> dict:
    sub_keys = jax.random.split(jax.random.key(seed), 19)
    seq_lens = jax.random.randint(sub_keys[1], (BATCH,), SEQ // 8, SEQ + 1, dtype=jnp.int32)
    seq_lens = seq_lens.at[0].set(SEQ).at[1].set(SEQ // 8)
    return {
        'x_in': draw_normal(sub_keys[0], (BATCH, SEQ, D), 1.0).astype(jnp.bfloat16),
        'seq_lens': seq_lens,
        'grad_out': draw_normal(sub_keys[2], (BATCH, SEQ, D), 1.0).astype(jnp.bfloat16),
        'ln1_gain': (1.0 + draw_normal(sub_keys[3], (D,), 0.3)).astype(jnp.bfloat16),
        'ln1_bias': draw_normal(sub_keys[4], (D,), 0.3).astype(jnp.bfloat16),
        'w_query': draw_normal(sub_keys[5], (D, HEADS, HEAD), D ** -0.5).astype(jnp.bfloat16),
        'b_query': draw_normal(sub_keys[6], (D,), 0.5).astype(jnp.bfloat16),
        'w_key': draw_normal(sub_keys[7], (D, HEADS, HEAD), D ** -0.5).astype(jnp.bfloat16),
        'b_key': draw_normal(sub_keys[8], (D,), 0.5).astype(jnp.bfloat16),
        'w_value': draw_normal(sub_keys[9], (D, HEADS, HEAD), D ** -0.5).astype(jnp.bfloat16),
        'b_value': draw_normal(sub_keys[10], (D,), 0.5).astype(jnp.bfloat16),
        'w_out': draw_normal(sub_keys[11], (HEADS, HEAD, D), D ** -0.5).astype(jnp.bfloat16),
        'b_out': draw_normal(sub_keys[12], (D,), 0.5).astype(jnp.bfloat16),
        'ln2_gain': (1.0 + draw_normal(sub_keys[13], (D,), 0.3)).astype(jnp.bfloat16),
        'ln2_bias': draw_normal(sub_keys[14], (D,), 0.3).astype(jnp.bfloat16),
        'w_fc1': draw_normal(sub_keys[15], (D, FF), D ** -0.5).astype(jnp.bfloat16),
        'b_fc1': draw_normal(sub_keys[16], (FF,), 0.5).astype(jnp.bfloat16),
        'w_fc2': draw_normal(sub_keys[17], (FF, D), FF ** -0.5).astype(jnp.bfloat16),
        'b_fc2': draw_normal(sub_keys[18], (D,), 0.5).astype(jnp.bfloat16),
    }


def normalize(values):
    row_mean = jnp.mean(values, axis=-1, keepdims=True)
    centered = values - row_mean
    variance = jnp.mean(centered * centered, axis=-1, keepdims=True)
    return centered * lax.rsqrt(variance + LN_EPS)


def layer_norm(values, ln_gain, ln_bias):
    return normalize(values) * ln_gain + ln_bias


def scaled_norm(values, ln_gain):
    return normalize(values) * ln_gain


def norm_vjp(values, ln_gain, d_norm):
    _, pullback = jax.vjp(scaled_norm, values, ln_gain)
    d_values, d_gain = pullback(d_norm)
    return d_values, d_gain, jnp.sum(d_norm, axis=0)


def gelu_exact(values):
    return jax.nn.gelu(values, approximate=False)


def rope_tables(seq_len, head_dim):
    inv_freq = ROPE_BASE ** (-jnp.arange(0, head_dim, 2, dtype=jnp.float32) / head_dim)
    angles = jnp.arange(seq_len, dtype=jnp.float32)[:, None] * inv_freq[None, :]
    angles = jnp.concatenate([angles, angles], axis=-1)
    return jnp.cos(angles)[:, None, :], jnp.sin(angles)[:, None, :]


def rotate_half(values):
    half_dim = values.shape[-1] // 2
    return jnp.concatenate([-values[..., half_dim:], values[..., :half_dim]], axis=-1)


def rotate_half_t(values):
    half_dim = values.shape[-1] // 2
    return jnp.concatenate([values[..., half_dim:], -values[..., :half_dim]], axis=-1)


def apply_rope(values, cos_tab, sin_tab):
    return values * cos_tab + rotate_half(values) * sin_tab


def apply_rope_t(grad_vals, cos_tab, sin_tab):
    return grad_vals * cos_tab + rotate_half_t(grad_vals * sin_tab)


def matmul_tn(lhs_arr, rhs_arr):
    return lax.dot_general(lhs_arr, rhs_arr, (((0,), (0,)), ((), ())), preferred_element_type=jnp.float32)


def matmul_nt(lhs_arr, rhs_arr):
    return lax.dot_general(lhs_arr, rhs_arr, (((1,), (1,)), ((), ())), preferred_element_type=jnp.float32)


def seq_probs(queries, key_vecs, key_row):
    scores = jnp.einsum('qhd,khd->hqk', queries.astype(jnp.float32), key_vecs.astype(jnp.float32))
    scores = jnp.where(key_row[None, None, :], scores, -1e30)
    return jax.nn.softmax(scores, axis=-1)


def seq_attention(operands):
    queries, key_vecs, val_vecs, key_row = operands
    attn_probs = seq_probs(queries, key_vecs, key_row).astype(jnp.bfloat16).astype(jnp.float32)
    context = jnp.einsum('hqk,khd->qhd', attn_probs, val_vecs.astype(jnp.float32))
    return context.astype(jnp.bfloat16)


def seq_attention_bwd(operands):
    queries, key_vecs, val_vecs, key_row, d_context = operands
    attn_probs = seq_probs(queries, key_vecs, key_row)
    d_ctx32 = d_context.astype(jnp.float32)
    d_vals = jnp.einsum('hqk,qhd->khd', attn_probs.astype(jnp.bfloat16).astype(jnp.float32), d_ctx32)
    d_probs = jnp.einsum('qhd,khd->hqk', d_ctx32, val_vecs.astype(jnp.float32))
    d_scores = attn_probs * (d_probs - jnp.sum(d_probs * attn_probs, axis=-1, keepdims=True))
    d_scores = d_scores.astype(jnp.bfloat16).astype(jnp.float32)
    d_queries = jnp.einsum('hqk,khd->qhd', d_scores, key_vecs.astype(jnp.float32))
    d_keys = jnp.einsum('hqk,qhd->khd', d_scores, queries.astype(jnp.float32))
    return d_queries, d_keys, d_vals


def reference(x_in, seq_lens, grad_out, ln1_gain, ln1_bias, w_query, b_query, w_key, b_key, w_value, b_value, w_out, b_out, ln2_gain, ln2_bias, w_fc1, b_fc1, w_fc2, b_fc2):
    tokens = BATCH * SEQ
    head_shape = (BATCH, SEQ, HEADS, HEAD)
    q_scale = HEAD ** -0.5
    cos_tab, sin_tab = rope_tables(SEQ, HEAD)
    key_mask = jnp.arange(SEQ)[None, :] < seq_lens[:, None]
    w_query_2d = w_query.reshape(D, D)
    w_key_2d = w_key.reshape(D, D)
    w_value_2d = w_value.reshape(D, D)
    w_out_2d = w_out.reshape(D, D)
    x_f32 = x_in.reshape(tokens, D).astype(jnp.float32)
    hidden_one = layer_norm(x_f32, ln1_gain.astype(jnp.float32), ln1_bias.astype(jnp.float32)).astype(jnp.bfloat16)
    q_lin = jnp.dot(hidden_one, w_query_2d, preferred_element_type=jnp.float32) + b_query.astype(jnp.float32)
    k_lin = jnp.dot(hidden_one, w_key_2d, preferred_element_type=jnp.float32) + b_key.astype(jnp.float32)
    v_lin = jnp.dot(hidden_one, w_value_2d, preferred_element_type=jnp.float32) + b_value.astype(jnp.float32)
    queries = apply_rope((q_lin * q_scale).reshape(head_shape), cos_tab, sin_tab).astype(jnp.bfloat16)
    key_vecs = apply_rope(k_lin.reshape(head_shape), cos_tab, sin_tab).astype(jnp.bfloat16)
    val_vecs = v_lin.astype(jnp.bfloat16).reshape(head_shape)
    context = lax.map(seq_attention, (queries, key_vecs, val_vecs, key_mask)).reshape(tokens, D)
    attn_proj = jnp.dot(context, w_out_2d, preferred_element_type=jnp.float32)
    resid_f32 = (x_f32 + attn_proj + b_out.astype(jnp.float32)).astype(jnp.bfloat16).astype(jnp.float32)
    hidden_two = layer_norm(resid_f32, ln2_gain.astype(jnp.float32), ln2_bias.astype(jnp.float32)).astype(jnp.bfloat16)
    pre_act = jnp.dot(hidden_two, w_fc1, preferred_element_type=jnp.float32) + b_fc1.astype(jnp.float32)
    gelu_out = gelu_exact(pre_act).astype(jnp.bfloat16)
    mlp_proj = jnp.dot(gelu_out, w_fc2, preferred_element_type=jnp.float32)
    y_out = (resid_f32 + mlp_proj + b_fc2.astype(jnp.float32)).astype(jnp.bfloat16).reshape(BATCH, SEQ, D)
    grad_flat = grad_out.reshape(tokens, D)
    grad_f32 = grad_flat.astype(jnp.float32)
    g_b_fc2 = jnp.sum(grad_f32, axis=0)
    g_w_fc2 = matmul_tn(gelu_out, grad_flat)
    _, gelu_pull = jax.vjp(gelu_exact, pre_act)
    d_pre = gelu_pull(matmul_nt(grad_flat, w_fc2))[0]
    d_pre_b = d_pre.astype(jnp.bfloat16)
    g_b_fc1 = jnp.sum(d_pre, axis=0)
    g_w_fc1 = matmul_tn(hidden_two, d_pre_b)
    d_resid, g_ln2_gain, g_ln2_bias = norm_vjp(resid_f32, ln2_gain.astype(jnp.float32), matmul_nt(d_pre_b, w_fc1))
    d_resid = d_resid + grad_f32
    d_resid_b = d_resid.astype(jnp.bfloat16)
    g_b_out = jnp.sum(d_resid, axis=0)
    g_w_out = matmul_tn(context, d_resid_b).reshape(HEADS, HEAD, D)
    d_context = matmul_nt(d_resid_b, w_out_2d).astype(jnp.bfloat16).reshape(head_shape)
    d_queries, d_keys, d_vals = lax.map(seq_attention_bwd, (queries, key_vecs, val_vecs, key_mask, d_context))
    d_q_lin = (apply_rope_t(d_queries, cos_tab, sin_tab) * q_scale).reshape(tokens, D)
    d_k_lin = apply_rope_t(d_keys, cos_tab, sin_tab).reshape(tokens, D)
    d_v_lin = d_vals.reshape(tokens, D)
    d_query_b = d_q_lin.astype(jnp.bfloat16)
    d_key_b = d_k_lin.astype(jnp.bfloat16)
    d_value_b = d_v_lin.astype(jnp.bfloat16)
    d_hidden_one = matmul_nt(d_query_b, w_query_2d) + matmul_nt(d_key_b, w_key_2d) + matmul_nt(d_value_b, w_value_2d)
    d_x_norm, g_ln1_gain, g_ln1_bias = norm_vjp(x_f32, ln1_gain.astype(jnp.float32), d_hidden_one)
    grad_x = (d_resid + d_x_norm).astype(jnp.bfloat16).reshape(BATCH, SEQ, D)
    return (y_out, grad_x, g_ln1_gain, g_ln1_bias,
            matmul_tn(hidden_one, d_query_b).reshape(D, HEADS, HEAD), jnp.sum(d_q_lin, axis=0),
            matmul_tn(hidden_one, d_key_b).reshape(D, HEADS, HEAD), jnp.sum(d_k_lin, axis=0),
            matmul_tn(hidden_one, d_value_b).reshape(D, HEADS, HEAD), jnp.sum(d_v_lin, axis=0),
            g_w_out, g_b_out, g_ln2_gain, g_ln2_bias, g_w_fc1, g_b_fc1, g_w_fc2, g_b_fc2)
```

```python
import functools

import jax
import jax.numpy as jnp
from jax import lax
from jax.experimental import pallas as pl
from jax.experimental.pallas import tpu as pltpu
from jax.sharding import PartitionSpec as P


F32 = jnp.float32
BF16 = jnp.bfloat16
LN_EPS = 1e-5
ROPE_BASE = 10000.0
MASKED = -1e30
D = 1024
HEADS = 16
HEAD = 64
FF = 4096
L = 256
LANES = 128
TP = 4
FSDP = 2
CHUNKS = 4
SWAP = [(0, 1), (1, 0)]
VMEM_LIMIT = 67043328
ROWS, SPLIT = P('fsdp'), P(('x', 'core', 'fsdp'))
HEADS_IN, HEADS_OUT = P('fsdp', ('x', 'core'), None), P(('x', 'core'), None, 'fsdp')
PARAM_SPECS = dict(ln1_gain=ROWS, ln1_bias=ROWS, w_query=HEADS_IN, b_query=SPLIT, w_key=HEADS_IN, b_key=SPLIT, w_value=HEADS_IN, b_value=SPLIT,
                   w_out=HEADS_OUT, b_out=ROWS, ln2_gain=ROWS, ln2_bias=ROWS, w_fc1=P('fsdp', ('x', 'core')), b_fc1=SPLIT,
                   w_fc2=P(('x', 'core'), 'fsdp'), b_fc2=ROWS)
PARAM_NAMES = tuple(PARAM_SPECS)
FSDP_VECTORS = tuple(name for name, spec in PARAM_SPECS.items() if spec is ROWS)
BOTH_VECTORS = tuple(name for name, spec in PARAM_SPECS.items() if spec is SPLIT)
BOTH = ('x', 'core', 'fsdp')

ERF_P = 0.3275911 * 0.7071067811865476
ERF_C = (0.254829592, -0.284496736, 1.421413741, -1.453152027, 1.061405429)
LOG2E = 1.4426950408889634
INV_SQRT_2PI = 0.3989422804014327


def nn(lhs, rhs):
    return lax.dot_general(lhs, rhs, (((1,), (0,)), ((), ())), preferred_element_type=F32)


def nt(lhs, rhs):
    return lax.dot_general(lhs, rhs, (((1,), (1,)), ((), ())), preferred_element_type=F32)


def tn(lhs, rhs):
    return lax.dot_general(lhs, rhs, (((0,), (0,)), ((), ())), preferred_element_type=F32)


def sum_groups(values):
    return values.reshape(values.shape[0] // 8, 8, values.shape[1]).sum(axis=0)


def standardize(values):
    centered = values - jnp.mean(values, axis=-1, keepdims=True)
    rstd = lax.rsqrt(jnp.mean(centered * centered, axis=-1, keepdims=True) + LN_EPS)
    return centered * rstd, rstd


def norm_input_grad(d_norm, gain, xhat, rstd):
    scaled = d_norm * gain
    mean_scaled = jnp.mean(scaled, axis=-1, keepdims=True)
    mean_dot = jnp.mean(scaled * xhat, axis=-1, keepdims=True)
    return rstd * (scaled - mean_scaled - xhat * mean_dot)


def gelu_and_grad(pre_act, d_act):
    t = 1.0 / (1.0 + ERF_P * jnp.abs(pre_act))
    gauss = jnp.exp2((-0.5 * LOG2E) * (pre_act * pre_act))
    poly = 0.5 * ERF_C[4]
    for coef in reversed(ERF_C[:4]):
        poly = poly * t + 0.5 * coef
    tail = poly * t * gauss
    cdf = jnp.where(pre_act < 0, tail, 1.0 - tail)
    slope = cdf + pre_act * (gauss * INV_SQRT_2PI)
    return pre_act * cdf, d_act * slope


def rope_tables():
    inv_freq = ROPE_BASE ** (-jnp.arange(0, HEAD, 2, dtype=F32) / HEAD)
    angles = jnp.arange(L, dtype=F32)[:, None] * inv_freq[None, :]
    cos, sin = jnp.cos(angles), jnp.sin(angles)
    wide_cos = jnp.concatenate([cos] * 4, axis=-1)
    wide_sin = jnp.concatenate([-sin, sin, -sin, sin], axis=-1)
    return wide_cos, wide_sin, cos.T, sin.T


def swap_halves(values):
    lane = lax.broadcasted_iota(jnp.int32, values.shape, 1)
    return jnp.where(lane % HEAD < HEAD // 2, pltpu.roll(values, LANES - HEAD // 2, 1), pltpu.roll(values, HEAD // 2, 1))


def only_head(tile, head):
    lane = lax.broadcasted_iota(jnp.int32, tile.shape, 1)
    return jnp.where((lane >= HEAD) == (head % 2 == 1), tile, jnp.zeros_like(tile))


def pair_lanes(head, base=0):
    first = base + head // 2 * LANES
    return slice(first, first + LANES)


def attn_fwd_body(seq_of, ready, meta, lens, x, b, gain, bias, cos, sin, w, h1_out, q_out, k_out, v_out, ctx_out, stats_out):
    seq_len = lens[seq_of(pl.program_id(0), meta)]
    xhat, _ = standardize(x[...].astype(F32))
    h1 = (xhat * gain[...] + bias[...]).astype(BF16)
    h1_out[...] = h1
    ready(0)
    for part, out in enumerate((q_out, k_out)):
        lin = nn(h1, w[:, part * D:(part + 1) * D]) + b[:, part * D:(part + 1) * D]
        for pair in range(D // LANES):
            lanes = slice(pair * LANES, (pair + 1) * LANES)
            tile = lin[:, lanes] * HEAD ** -0.5 if part == 0 else lin[:, lanes]
            out[:, lanes] = (tile * cos[...] + swap_halves(tile) * sin[...]).astype(BF16)
    v_out[...] = (nn(h1, w[:, 2 * D:]) + b[:, 2 * D:]).astype(BF16)
    key_ok = lax.broadcasted_iota(jnp.int32, (L, L), 1) < seq_len

    def scores_of(head):
        return nt(only_head(q_out[:, pair_lanes(head)], head), k_out[:, pair_lanes(head)])

    ahead = 2
    scores = [scores_of(head) for head in range(ahead)]
    lane = lax.broadcasted_iota(jnp.int32, (L, LANES), 1)
    stats = jnp.zeros((L, LANES), F32)
    ctx = None
    for head in range(HEADS):
        if head + ahead < HEADS:
            scores.append(scores_of(head + ahead))
        masked = jnp.where(key_ok, scores[head], MASKED)
        scores[head] = None
        top = jnp.max(masked, axis=1, keepdims=True)
        weights = jnp.exp(masked - top)
        total = jnp.sum(weights, axis=1, keepdims=True)
        inverse = 1.0 / total
        stats = jnp.where(lane == head, top, jnp.where(lane == HEADS + head, inverse, stats))
        part = nn((weights * inverse).astype(BF16), only_head(v_out[:, pair_lanes(head)], head))
        ctx = part if head % 2 == 0 else ctx + part
        if head % 2 == 1:
            ctx_out[:, pair_lanes(head)] = ctx.astype(BF16)
    stats_out[0] = stats.T[:2 * HEADS]


def mlp_body(ready, meta, x, ctx, dy, bo, gain, bias, b1, b2, rows_in, cols_in, wo, w1, w2, y_out, da_out, dctx_out, h2_out, act_out, du_out, dab_out, row_sums, col_sums):
    cols = D

    @pl.when(pl.program_id(0) == 0)
    def _():
        row_sums[...] = rows_in[...]
        col_sums[...] = cols_in[...]

    ready(0)
    resid = (x[...].astype(F32) + nn(ctx[...], wo[...]) + bo[...]).astype(BF16).astype(F32)
    xhat, rstd = standardize(resid)
    h2 = (xhat * gain[...] + bias[...]).astype(BF16)
    h2_out[...] = h2
    ready(1)
    ready(2)
    y_acc = jnp.zeros((L, D), F32)
    dh_acc = jnp.zeros((L, D), F32)
    for step in range(FF // cols):
        sl = slice(step * cols, (step + 1) * cols)
        pre_act = nn(h2, w1[:, sl]) + b1[:, sl]
        act, du = gelu_and_grad(pre_act, nt(dy[...], w2[sl, :]))
        col_sums[:, sl] += sum_groups(du)
        act, du = act.astype(BF16), du.astype(BF16)
        act_out[:, sl] = act
        du_out[:, sl] = du
        y_acc += nn(act, w2[sl, :])
        dh_acc += nt(du, w1[:, sl])
    y_out[...] = (resid + y_acc + b2[...]).astype(BF16)
    dy_f32 = dy[...].astype(F32)
    da = norm_input_grad(dh_acc, gain[...], xhat, rstd) + dy_f32
    da_out[...] = da
    da_b = da.astype(BF16)
    dab_out[...] = da_b
    dctx_out[...] = nt(da_b, wo[...]).astype(BF16)
    row_sums[0] += sum_groups(dh_acc * xhat)
    row_sums[1] += sum_groups(dh_acc)
    row_sums[2] += sum_groups(da)
    row_sums[3] += sum_groups(dy_f32)


def attn_bwd_body(ready, meta, lens, x, q, k, v, dctx, stats, da, gain, cos, sin, cos_t, sin_t, rows_in, q_in, kv_in, w, dx_out, dqkv_out, row_sums, q_sums, kv_sums, k_t, dq_t):
    @pl.when(pl.program_id(0) == 0)
    def _():
        row_sums[...] = rows_in[...]
        q_sums[...] = q_in[...]
        kv_sums[...] = kv_in[...]

    seq_len = lens[meta[0] + pl.program_id(0)]
    k_t[...] = k[...].T
    key_ok = lax.broadcasted_iota(jnp.int32, (L, L), 0) < seq_len
    half = HEAD // 2

    def products(head):
        lanes = pair_lanes(head)
        return nt(only_head(k[:, lanes], head), q[:, lanes]), nt(only_head(v[:, lanes], head), dctx[:, lanes])

    def softmax_grad(head, scores, d_probs):
        probs = jnp.exp(jnp.where(key_ok, scores, MASKED) - stats[0, head:head + 1, :]) * stats[0, HEADS + head:HEADS + head + 1, :]
        d_scores = probs * (d_probs - jnp.sum(d_probs * probs, axis=0, keepdims=True))
        return probs.astype(BF16), d_scores.astype(BF16)

    pending = {}

    def gradients(head, probs, d_scores):
        lanes = pair_lanes(head)
        dv = nn(probs, only_head(dctx[:, lanes], head))
        dk = nn(d_scores, only_head(q[:, lanes], head))
        dq = nn(k_t[head * HEAD:(head + 1) * HEAD, :], d_scores)
        low = (dq[:half] * cos_t[...] + dq[half:] * sin_t[...]) * HEAD ** -0.5
        high = (dq[half:] * cos_t[...] - dq[:half] * sin_t[...]) * HEAD ** -0.5
        for first, part in ((head * HEAD, low), (head * HEAD + half, high)):
            rows = slice(first, first + half)
            q_sums[rows, :] += part[:, :LANES] + part[:, LANES:]
            dq_t[rows, :] = part.astype(BF16)
        if head % 2 == 0:
            pending[head // 2] = dv, dk
            return
        dv_first, dk_first = pending.pop(head // 2)
        dv, dk = dv_first + dv, dk_first + dk
        dk = dk * cos[...] - swap_halves(dk) * sin[...]
        kv_sums[0, :, lanes] += sum_groups(dk)
        kv_sums[1, :, lanes] += sum_groups(dv)
        dqkv_out[:, pair_lanes(head, D)] = dk.astype(BF16)
        dqkv_out[:, pair_lanes(head, 2 * D)] = dv.astype(BF16)

    ahead = 2
    first = [products(head) for head in range(ahead)]
    second = None
    for head in range(HEADS):
        if head + ahead < HEADS:
            first.append(products(head + ahead))
        if second is not None:
            gradients(head - 1, *second)
        second = softmax_grad(head, *first[head])
        first[head] = None
    gradients(HEADS - 1, *second)
    dqkv_out[:, :D] = dq_t[...].T
    ready(0)
    dh = nt(dqkv_out[...], w[...])
    xhat, rstd = standardize(x[...].astype(F32))
    dx_out[...] = (da[...] + norm_input_grad(dh, gain[...], xhat, rstd)).astype(BF16)
    row_sums[0] += sum_groups(dh * xhat)
    row_sums[1] += sum_groups(dh)


def weight_grad_body(store, meta, lhs, rhs, *rest):
    partner, out = rest if len(rest) == 2 else (None, rest[0])
    acc = tn(lhs[...], rhs[...])
    k_step = pl.program_id(1)

    @pl.when(k_step == 0)
    def _():
        for at, part in store(acc):
            out[at] = part if partner is None else part + partner[at]

    @pl.when(k_step > 0)
    def _():
        for at, part in store(acc):
            out[at] += part


class Placing:
    def __init__(self, pieces, target, chunk):
        self.pieces, self.target, self.chunk = pieces, target, chunk

    def moves(self, steps):
        return 1 << (steps.bit_length() - 1)

    def rows_per_step(self, steps):
        return self.pieces[0].shape[0] // self.moves(steps)

    def scratch(self, steps):
        n = len(self.pieces)
        return [pltpu.VMEM((2, n, self.rows_per_step(steps), D), BF16), pltpu.SemaphoreType.DMA((2, n)), pltpu.SemaphoreType.DMA((2, n))]

    def hooks(self, steps, step, meta, pieces, target, buf, in_sem, out_sem):
        rows = self.rows_per_step(steps)
        total = self.pieces[0].shape[0]

        def fetch(j, s):
            return pltpu.make_async_copy(pieces[j].at[pl.ds(s * rows, rows)], buf.at[s % 2, j], in_sem.at[s % 2, j])

        def put(j, s):
            row = pl.multiple_of((meta[3] * TP + jnp.bitwise_xor(meta[1], j)) * total + s * rows, rows)
            return pltpu.make_async_copy(buf.at[s % 2, j], target.at[pl.ds(row, rows)], out_sem.at[s % 2, j])

        every = range(len(self.pieces))
        moves = self.moves(steps)

        def before():
            @pl.when((step >= 2) & (step < moves))
            def _():
                for j in every:
                    put(j, step - 2).wait()

            @pl.when(step < moves)
            def _():
                for j in every:
                    fetch(j, step).start()

        def after():
            @pl.when(step < moves)
            def _():
                for j in every:
                    fetch(j, step).wait()
                    put(j, step).start()

            @pl.when(step == moves - 1)
            def _():
                for j in every:
                    put(j, step - 1).wait()
                    put(j, step).wait()

        return before, after


def call(body, grid, scalars, streams, consts, weights, outs, prior, scratch, flops, n_bytes, placing=None, hand_on=False):
    steps = 1
    for size in grid:
        steps *= size

    def whole(array):
        return pl.BlockSpec(array.shape, lambda *_: (0,) * array.ndim, pipeline_mode=pl.Buffered(1))

    anywhere = pl.BlockSpec(memory_space=pl.ANY)
    n_scalar, n_stream, n_const, n_weight, n_out = len(scalars), len(streams), len(consts), len(weights), len(outs)
    operands = [a for a, _, _ in streams] + list(consts) + [a for a, _, _ in weights] + list(prior.values())
    in_specs = [pl.BlockSpec(block, index) for _, block, index in streams] + [whole(a) for a in consts] + [anywhere] * (n_weight + len(prior))
    aliases = {n_scalar + n_stream + n_const + n_weight + i: out for i, out in enumerate(prior)}
    out_specs = [pl.BlockSpec(block, index) for _, _, block, index in outs]
    out_shape = [jax.ShapeDtypeStruct(shape, dtype) for shape, dtype, _, _ in outs]
    n_hand = n_weight if hand_on else 0
    n_piece = 0
    scratches = [pltpu.VMEM(shape, BF16) for _, shape, _ in weights] + [pltpu.SemaphoreType.DMA((len(moves),)) for _, _, moves in weights]
    if placing is not None:
        n_piece = len(placing.pieces)
        aliases[n_scalar + len(operands) + n_piece] = n_out
        operands += list(placing.pieces) + [placing.target]
        in_specs += [anywhere] * (n_piece + 1)
        out_specs.append(anywhere)
        out_shape.append(jax.ShapeDtypeStruct(placing.target.shape, placing.target.dtype))
        scratches += placing.scratch(steps)
    out_specs += [anywhere] * n_hand
    out_shape += [jax.ShapeDtypeStruct(shape, BF16) for _, shape, _ in weights[:n_hand]]
    scratches += [pltpu.SemaphoreType.DMA((n_hand,))] * bool(n_hand) + scratch

    def kernel(*refs):
        refs = list(refs)

        def take(n):
            taken = refs[:n]
            del refs[:n]
            return taken

        scalar_refs, stream_refs, const_refs, weight_refs = take(n_scalar), take(n_stream), take(n_const), take(n_weight)
        take(len(prior))
        piece_refs = take(n_piece)
        if placing is not None:
            take(1)
        out_refs = take(n_out)
        target = take(1) if placing is not None else None
        handed = take(n_hand)
        held, sems = take(n_weight), take(n_weight)
        step = pl.program_id(0)
        for axis in range(1, len(grid)):
            step = step * grid[axis] + pl.program_id(axis)

        copies = [[pltpu.make_async_copy(ref.at[source] if source else ref, to.at[dest] if dest else to, sem.at[i]) for i, (source, dest) in enumerate(moves)]
                  for (_, _, moves), ref, to, sem in zip(weights, weight_refs, held, sems)]

        def ready(which):
            @pl.when(step == 0)
            def _():
                for copy in copies[which]:
                    copy.wait()

        if n_weight:
            @pl.when(step == 0)
            def _():
                for copy in sum(copies, []):
                    copy.start()

        if placing is not None:
            before, after = placing.hooks(steps, step, scalar_refs[0], piece_refs, target[0], *take(3))
            before()
        if n_hand:
            hand_sem, = take(1)
            hands = [pltpu.make_async_copy(ref, to, hand_sem.at[i]) for i, (ref, to) in enumerate(zip(held, handed))]

            @pl.when(step == 1)
            def _():
                for copy in hands:
                    copy.start()

        body(*([ready] if n_weight else []), *scalar_refs, *stream_refs, *const_refs, *held, *out_refs, *refs)
        if placing is not None:
            after()
        if n_hand:
            @pl.when(step == steps - 1)
            def _():
                for copy in hands:
                    copy.wait()

    return pl.pallas_call(
        kernel,
        grid_spec=pltpu.PrefetchScalarGridSpec(num_scalar_prefetch=n_scalar, grid=grid, in_specs=in_specs, out_specs=out_specs, scratch_shapes=scratches),
        out_shape=out_shape, input_output_aliases=aliases,
        compiler_params=pltpu.CompilerParams(dimension_semantics=("arbitrary",) * len(grid), vmem_limit_bytes=VMEM_LIMIT),
        cost_estimate=pl.CostEstimate(flops=flops, bytes_accessed=n_bytes, transcendentals=0))(*scalars, *operands)


def uninitialized(shape, dtype):
    return pl.pallas_call(lambda out: None, out_specs=pl.BlockSpec(memory_space=pl.ANY),
                          out_shape=jax.ShapeDtypeStruct(shape, dtype), name="uninitialized")()


def send_around(block):
    across = lax.ppermute(block, 'x', SWAP)
    beside = lax.ppermute(block, 'core', SWAP)
    diagonal = lax.ppermute(across, 'core', SWAP)
    return [block, beside, across, diagonal]


def block_moves(tp_dim, tp_size, fsdp_dim, fsdp_size):
    moves = []
    for t in range(TP):
        for f in range(FSDP):
            dest = [None, None]
            dest[tp_dim] = pl.ds(t * tp_size, tp_size)
            dest[fsdp_dim] = pl.ds(f * fsdp_size, fsdp_size)
            moves.append(((t * FSDP + f,), tuple(dest)))
    return moves


def device_layer(x_in, seq_lens, grad_out, *weight_shards):
    p = dict(zip(PARAM_NAMES, weight_shards))
    n_seq = x_in.shape[0]
    rows_all = n_seq * L
    tp_index = (lax.axis_index('x') * 2 + lax.axis_index('core')).astype(jnp.int32)
    x_rows = x_in.reshape(rows_all, D)
    dy_rows = grad_out.reshape(rows_all, D)
    rows_mine = rows_all // TP
    rows_chunk = rows_mine // CHUNKS
    rows_part = rows_all // CHUNKS
    seqs_chunk = rows_chunk // L

    vec_names = FSDP_VECTORS + BOTH_VECTORS
    gather = functools.partial(lax.all_gather, axis_name=BOTH, axis=0, tiled=False)
    vec_all = gather(jnp.concatenate([p[name] for name in vec_names])).reshape(TP, FSDP, -1)
    vec, place = {}, 0
    for name in vec_names:
        size = p[name].shape[0]
        part = vec_all[:, :, place:place + size]
        vec[name] = (part[0] if name in FSDP_VECTORS else part).reshape(1, -1).astype(F32)
        place += size
    qkv_blocks = gather(jnp.stack([p[name].reshape(D // 2, D // 4) for name in ('w_query', 'w_key', 'w_value')]))
    qkv_moves = [((owner[0], part), (dest[0], pl.ds(part * D + dest[1].start, D // 4)))
                 for owner, dest in block_moves(1, D // 4, 0, D // 2) for part in range(3)]
    w_qkv = qkv_blocks, (D, 3 * D), qkv_moves
    w_out = gather(p['w_out'].reshape(D // 4, D // 2)), (D, D), block_moves(0, D // 4, 1, D // 2)
    w_fc1 = gather(p['w_fc1']), (D, FF), block_moves(1, FF // 4, 0, D // 2)
    w_fc2 = gather(p['w_fc2']), (FF, D), block_moves(0, FF // 4, 1, D // 2)
    b_qkv = jnp.concatenate([vec['b_query'], vec['b_key'], vec['b_value']], axis=1)
    cos, sin, cos_t, sin_t = rope_tables()

    y_full = uninitialized((rows_all, D), BF16)
    dx_full = uninitialized((rows_all, D), BF16)

    def shared(i, meta, *_):
        return meta[0] + i, 0

    def local(i, *_):
        return i, 0

    def kept(i, meta, *_):
        return meta[2] + i, 0

    def seq3(i, *_):
        return i, 0, 0

    def keep(width):
        return (rows_mine, width), BF16, (L, width), kept

    def pass_on(width, dtype=BF16):
        return (rows_chunk, width), dtype, (L, width), local

    def total(*shape):
        return shape, F32, shape, lambda i, *_: (0,) * len(shape)

    prior_m = {3: uninitialized((rows_mine, D), BF16), 4: uninitialized((rows_mine, FF), BF16), 5: uninitialized((rows_mine, FF), BF16), 6: uninitialized((rows_mine, D), BF16)}
    prior_b = {1: uninitialized((rows_mine, 3 * D), BF16)}
    grid = (seqs_chunk,)
    mlp, bwd = [None] * CHUNKS, [None] * CHUNKS
    y_pieces, dx_pieces = [None] * CHUNKS, [None] * CHUNKS
    x_stream = (x_rows, (L, D), shared)

    def meta_of(c, placing=None, core=0):
        return jnp.stack([jnp.asarray(value, jnp.int32) for value in (
            c * (n_seq // CHUNKS) + tp_index * seqs_chunk, tp_index, c * seqs_chunk, placing.chunk if placing else 0, core)])

    def spread(i, meta, *_):
        return i // seqs_chunk * (n_seq // CHUNKS) + meta[0] + i % seqs_chunk

    whole_move = [(None, None)]
    h1, q, k, v, ctx, stats, w_qkv = call(
        functools.partial(attn_fwd_body, spread), (rows_mine // L,), [meta_of(0), seq_lens],
        [(x_rows, (L, D), lambda i, meta, *_: (spread(i, meta), 0))],
        [b_qkv, vec['ln1_gain'], vec['ln1_bias'], cos, sin], [w_qkv],
        [((rows_mine, D), BF16, (L, D), local)] * 5 + [((rows_mine // L, 2 * HEADS, L), F32, (1, 2 * HEADS, L), seq3)], {}, [],
        rows_mine * (6 * D * D + 64 * L * D), rows_mine * D * 12 + 6 * D * D, hand_on=True)

    arranged = []
    sums_m = [jnp.zeros(shape, F32) for shape in ((4, 8, D), (8, FF))]
    sums_b = [jnp.zeros(shape, F32) for shape in ((2, 8, D), (D, LANES), (2, 8, D))]

    def run_mlp(c, placing=None):
        out = call(
            mlp_body, grid, [meta_of(c, placing)],
            [x_stream, (ctx, (L, D), kept), (dy_rows, (L, D), shared)],
            [vec['b_out'], vec['ln2_gain'], vec['ln2_bias'], vec['b_fc1'], vec['b_fc2']] + sums_m, arranged or [w_out, w_fc1, w_fc2],
            [pass_on(D), pass_on(D, F32), pass_on(D), keep(D), keep(FF), keep(FF), keep(D), total(4, 8, D), total(8, FF)],
            prior_m, [], rows_chunk * (4 * D * D + 16 * D * FF), rows_chunk * (D * 20 + FF * 4) + 18 * D * D, placing, hand_on=not arranged)
        if not arranged:
            arranged.extend((array, array.shape, whole_move) for array in out[9:])
        prior_m.update({i: out[i] for i in prior_m})
        mlp[c] = out
        sums_m[:] = out[7:9]
        y_pieces[c] = send_around(out[0])
        return out[9:] if placing else ()

    def run_bwd(c, placing=None):
        saved = [(array, (L, D), kept) for array in (q, k, v)] + [(mlp[c][2], (L, D), local)]
        out = call(
            attn_bwd_body, grid, [meta_of(c, placing), seq_lens],
            [x_stream] + saved + [(stats, (1, 2 * HEADS, L), lambda i, meta, *_: (meta[2] + i, 0, 0)), (mlp[c][1], (L, D), local)],
            [vec['ln1_gain'], cos, sin, cos_t, sin_t] + sums_b, [(w_qkv, w_qkv.shape, whole_move)],
            [pass_on(D), keep(3 * D), total(2, 8, D), total(D, LANES), total(2, 8, D)], prior_b,
            [pltpu.VMEM((D, L), BF16), pltpu.VMEM((D, L), BF16)],
            rows_chunk * (6 * D * D + 160 * L * D), rows_chunk * D * 22 + 6 * D * D, placing)
        prior_b.update({1: out[1]})
        bwd[c] = out
        sums_b[:] = out[2:5]
        dx_pieces[c] = send_around(out[0])
        return out[5:]

    def weight_grad(lhs, rhs, lhs_index, rhs_index, n_out, size, block, out_index, store, placing=None):
        return call(
            functools.partial(weight_grad_body, store), (n_out, rows_mine // rows_chunk), [meta_of(0, placing)],
            [(lhs, (rows_chunk, D), lhs_index), (rhs, (rows_chunk, D), rhs_index)], [], [],
            [((2, FSDP, 2) + size, F32, block, out_index)], {}, [],
            2 * n_out * rows_mine * D * D, n_out * rows_mine * D * 4, placing)

    def swap_halves_along(axis, halves):
        index = lax.axis_index(axis)
        theirs = lax.ppermute(lax.dynamic_index_in_dim(halves, 1 - index, keepdims=False), axis, SWAP)
        return lax.dynamic_index_in_dim(halves, index, keepdims=False) + theirs

    def scatter(grad):
        size = grad.shape[3:]
        pair = lax.psum_scatter(grad.reshape(-1, size[-1]), ('core', 'fsdp'), scatter_dimension=0, tiled=True).reshape((2,) + size)
        return swap_halves_along('x', pair)

    def by_row(n, k, *_):
        return k, 0

    def by_row_and_part(n, k, *_):
        return k, n

    def by_chunk(n, k, meta):
        return k * TP + meta[1], 0

    half, quarter = D // 2, D // 4
    owners = [(t, f) for t in range(TP) for f in range(FSDP)]

    def store_fc2(acc):
        return [((0, f, 0), acc[:, f * half:(f + 1) * half]) for f in range(FSDP)]

    def store_fc1(acc):
        return [((0, f, 0), acc[f * half:(f + 1) * half]) for f in range(FSDP)]

    def store_qkv(acc):
        return [((t % 2, f, t // 2, 0), acc[f * half:(f + 1) * half, t * quarter:(t + 1) * quarter]) for t, f in owners]

    def store_out(acc):
        return [((t % 2, f, t // 2), acc[t * quarter:(t + 1) * quarter, f * half:(f + 1) * half]) for t, f in owners]

    def store_v(acc):
        return [((t // 2, t % 2, f), acc[f * half:(f + 1) * half, t * quarter:(t + 1) * quarter]) for t, f in owners]

    def owner_block(n, k, *_):
        return n % 2, 0, n // 2, 0, 0

    grads = {}
    last = CHUNKS - 1
    run_mlp(0)
    run_bwd(0)
    run_mlp(1)
    run_bwd(1)
    y_full, = run_mlp(2, Placing(y_pieces[0], y_full, 0))
    dx_full, = run_mlp(3, Placing(dx_pieces[0], dx_full, 0))
    h2, act, du, da_b = mlp[last][3:7]
    grads['w_fc1'] = scatter(weight_grad(h2, du, by_row, by_row_and_part, TP, (half, FF // 4), (1, FSDP, 1, half, FF // 4), owner_block, store_fc1)[0])
    y_full, = run_bwd(2, Placing(y_pieces[1], y_full, 1))
    grad, dx_full = weight_grad(act, dy_rows, by_row_and_part, by_chunk, TP, (FF // 4, half), (1, FSDP, 1, FF // 4, half), owner_block, store_fc2,
                                Placing(dx_pieces[1], dx_full, 1))
    grads['w_fc2'] = scatter(grad)
    y_full, = run_bwd(3, Placing(y_pieces[2], y_full, 2))
    dqkv = bwd[last][1]
    grad, y_full = weight_grad(h1, dqkv, by_row, by_row_and_part, 2, (2, half, quarter), (2, FSDP, 2, 1, half, quarter),
                               lambda n, k, *_: (0, 0, 0, n, 0, 0), store_qkv, Placing(y_pieces[last], y_full, last))
    qk_grad = scatter(grad)
    grad, dx_full = weight_grad(ctx, da_b, by_row, by_row, 1, (quarter, half), (2, FSDP, 2, quarter, half), lambda n, k, *_: (0,) * 5, store_out,
                                Placing(dx_pieces[2], dx_full, 2))
    for axis in ('core', 'fsdp', 'x'):
        grad = swap_halves_along(axis, grad)
    grads['w_out'] = grad.reshape(p['w_out'].shape)
    grad, = weight_grad(h1, dqkv, by_row, lambda n, k, *_: (k, 2), 1, (half, quarter), (2, FSDP, 2, half, quarter), lambda n, k, *_: (0,) * 5, store_v)
    v_grad = lax.psum_scatter(grad.reshape(TP * FSDP, half, quarter), BOTH, scatter_dimension=0, tiled=False)
    for name, grad in zip(('w_query', 'w_key', 'w_value'), (qk_grad[0], qk_grad[1], v_grad)):
        grads[name] = grad.reshape(p[name].shape)
    placing = Placing(dx_pieces[last], dx_full, last)
    dx_full, = call(lambda meta: None, (8,), [meta_of(0, placing)], [], [], [], [], {}, [], 10 ** 9, rows_part * D * 4, placing)

    rows_b, q_sums, kv_sums = sums_b
    rows = jnp.concatenate([rows_b, sums_m[0], kv_sums]).sum(axis=1)
    flat = jnp.concatenate([rows.reshape(-1), q_sums.sum(axis=1), sums_m[1].sum(axis=0)])
    for axis in ('core', 'fsdp', 'x'):
        flat = flat + lax.ppermute(flat, axis, SWAP)
    n_rows = len(FSDP_VECTORS)
    fsdp_index = lax.axis_index('fsdp')
    owner = tp_index * FSDP + fsdp_index
    by_fsdp = lax.dynamic_index_in_dim(flat[:n_rows * D].reshape(n_rows, FSDP, -1), fsdp_index, axis=1, keepdims=False)
    by_owner = lax.dynamic_index_in_dim(flat[n_rows * D:(n_rows + 3) * D].reshape(3, TP * FSDP, -1), owner, axis=1, keepdims=False)
    by_owner_ff = lax.dynamic_index_in_dim(flat[(n_rows + 3) * D:].reshape(TP * FSDP, -1), owner, keepdims=False)
    for name, grad in zip(('ln1_gain', 'ln1_bias', 'ln2_gain', 'ln2_bias', 'b_out', 'b_fc2'), by_fsdp):
        grads[name] = grad
    grads.update(b_key=by_owner[0], b_value=by_owner[1], b_query=by_owner[2], b_fc1=by_owner_ff)
    return (y_full.reshape(x_in.shape), dx_full.reshape(x_in.shape)) + tuple(grads[name] for name in PARAM_NAMES)


def solution(mesh):
    split = jax.sharding.Mesh(mesh.devices.reshape(FSDP, 2, 2), ('fsdp', 'x', 'core'))
    act_spec = P('fsdp', None, None)
    weight_specs = tuple(PARAM_SPECS.values())
    return jax.shard_map(device_layer, mesh=split, in_specs=(act_spec, ROWS, act_spec) + weight_specs,
                         out_specs=(act_spec, act_spec) + weight_specs, check_vma=False)
```

```python
import functools

import jax
import jax.numpy as jnp
from jax import lax
from jax.experimental import pallas as pl
from jax.experimental.pallas import tpu as pltpu
from jax.sharding import PartitionSpec as P


F32 = jnp.float32
BF16 = jnp.bfloat16
LN_EPS = 1e-5
ROPE_BASE = 10000.0
MASKED = -1e30
D = 1024
HEADS = 16
HEAD = 64
FF = 4096
L = 256
LANES = 128
TP = 4
FSDP = 2
CHUNKS = 4
SWAP = [(0, 1), (1, 0)]
VMEM_LIMIT = 67043328
ROWS, SPLIT = P('fsdp'), P(('x', 'core', 'fsdp'))
HEADS_IN, HEADS_OUT = P('fsdp', ('x', 'core'), None), P(('x', 'core'), None, 'fsdp')
PARAM_SPECS = dict(ln1_gain=ROWS, ln1_bias=ROWS, w_query=HEADS_IN, b_query=SPLIT, w_key=HEADS_IN, b_key=SPLIT, w_value=HEADS_IN, b_value=SPLIT,
                   w_out=HEADS_OUT, b_out=ROWS, ln2_gain=ROWS, ln2_bias=ROWS, w_fc1=P('fsdp', ('x', 'core')), b_fc1=SPLIT,
                   w_fc2=P(('x', 'core'), 'fsdp'), b_fc2=ROWS)
PARAM_NAMES = tuple(PARAM_SPECS)
FSDP_VECTORS = tuple(name for name, spec in PARAM_SPECS.items() if spec is ROWS)
BOTH_VECTORS = tuple(name for name, spec in PARAM_SPECS.items() if spec is SPLIT)
BOTH = ('x', 'core', 'fsdp')

ERF_P = 0.3275911 * 0.7071067811865476
ERF_C = (0.254829592, -0.284496736, 1.421413741, -1.453152027, 1.061405429)
LOG2E = 1.4426950408889634
INV_SQRT_2PI = 0.3989422804014327


def nn(lhs, rhs):
    return lax.dot_general(lhs, rhs, (((1,), (0,)), ((), ())), preferred_element_type=F32)


def nt(lhs, rhs):
    return lax.dot_general(lhs, rhs, (((1,), (1,)), ((), ())), preferred_element_type=F32)


def tn(lhs, rhs):
    return lax.dot_general(lhs, rhs, (((0,), (0,)), ((), ())), preferred_element_type=F32)


def sum_groups(values):
    return values.reshape(values.shape[0] // 8, 8, values.shape[1]).sum(axis=0)


def standardize(values):
    centered = values - jnp.mean(values, axis=-1, keepdims=True)
    rstd = lax.rsqrt(jnp.mean(centered * centered, axis=-1, keepdims=True) + LN_EPS)
    return centered * rstd, rstd


def norm_input_grad(d_norm, gain, xhat, rstd):
    scaled = d_norm * gain
    mean_scaled = jnp.mean(scaled, axis=-1, keepdims=True)
    mean_dot = jnp.mean(scaled * xhat, axis=-1, keepdims=True)
    return rstd * (scaled - mean_scaled - xhat * mean_dot)


def gelu_and_grad(pre_act, d_act):
    t = 1.0 / (1.0 + ERF_P * jnp.abs(pre_act))
    gauss = jnp.exp2((-0.5 * LOG2E) * (pre_act * pre_act))
    poly = 0.5 * ERF_C[4]
    for coef in reversed(ERF_C[:4]):
        poly = poly * t + 0.5 * coef
    tail = poly * t * gauss
    cdf = jnp.where(pre_act < 0, tail, 1.0 - tail)
    slope = cdf + pre_act * (gauss * INV_SQRT_2PI)
    return pre_act * cdf, d_act * slope


def rope_tables():
    inv_freq = ROPE_BASE ** (-jnp.arange(0, HEAD, 2, dtype=F32) / HEAD)
    angles = jnp.arange(L, dtype=F32)[:, None] * inv_freq[None, :]
    cos, sin = jnp.cos(angles), jnp.sin(angles)
    wide_cos = jnp.concatenate([cos] * 4, axis=-1)
    wide_sin = jnp.concatenate([-sin, sin, -sin, sin], axis=-1)
    return wide_cos, wide_sin, cos.T, sin.T


def swap_halves(values):
    lane = lax.broadcasted_iota(jnp.int32, values.shape, 1)
    return jnp.where(lane % HEAD < HEAD // 2, pltpu.roll(values, LANES - HEAD // 2, 1), pltpu.roll(values, HEAD // 2, 1))


def only_head(tile, head):
    lane = lax.broadcasted_iota(jnp.int32, tile.shape, 1)
    return jnp.where((lane >= HEAD) == (head % 2 == 1), tile, jnp.zeros_like(tile))


def pair_lanes(head, base=0):
    first = base + head // 2 * LANES
    return slice(first, first + LANES)


def attn_fwd_body(seq_of, ready, meta, lens, x, b, gain, bias, cos, sin, w, h1_out, q_out, k_out, v_out, ctx_out, stats_out):
    seq_len = lens[seq_of(pl.program_id(0), meta)]
    xhat, _ = standardize(x[...].astype(F32))
    h1 = (xhat * gain[...] + bias[...]).astype(BF16)
    h1_out[...] = h1
    ready(0)
    for part, out in enumerate((q_out, k_out)):
        lin = nn(h1, w[:, part * D:(part + 1) * D]) + b[:, part * D:(part + 1) * D]
        for pair in range(D // LANES):
            lanes = slice(pair * LANES, (pair + 1) * LANES)
            tile = lin[:, lanes] * HEAD ** -0.5 if part == 0 else lin[:, lanes]
            out[:, lanes] = (tile * cos[...] + swap_halves(tile) * sin[...]).astype(BF16)
    v_out[...] = (nn(h1, w[:, 2 * D:]) + b[:, 2 * D:]).astype(BF16)
    key_ok = lax.broadcasted_iota(jnp.int32, (L, L), 1) < seq_len

    def scores_of(head):
        return nt(only_head(q_out[:, pair_lanes(head)], head), k_out[:, pair_lanes(head)])

    ahead = 2
    scores = [scores_of(head) for head in range(ahead)]
    lane = lax.broadcasted_iota(jnp.int32, (L, LANES), 1)
    stats = jnp.zeros((L, LANES), F32)
    ctx = None
    for head in range(HEADS):
        if head + ahead < HEADS:
            scores.append(scores_of(head + ahead))
        masked = jnp.where(key_ok, scores[head], MASKED)
        scores[head] = None
        top = jnp.max(masked, axis=1, keepdims=True)
        weights = jnp.exp(masked - top)
        total = jnp.sum(weights, axis=1, keepdims=True)
        inverse = 1.0 / total
        stats = jnp.where(lane == head, top, jnp.where(lane == HEADS + head, inverse, stats))
        part = nn((weights * inverse).astype(BF16), only_head(v_out[:, pair_lanes(head)], head))
        ctx = part if head % 2 == 0 else ctx + part
        if head % 2 == 1:
            ctx_out[:, pair_lanes(head)] = ctx.astype(BF16)
    stats_out[0] = stats.T[:2 * HEADS]


def mlp_body(ready, meta, x, ctx, dy, bo, gain, bias, b1, b2, rows_in, cols_in, wo, w1, w2, y_out, da_out, dctx_out, h2_out, act_out, du_out, dab_out, row_sums, col_sums):
    cols = D

    @pl.when(pl.program_id(0) == 0)
    def _():
        row_sums[...] = rows_in[...]
        col_sums[...] = cols_in[...]

    ready(0)
    resid = (x[...].astype(F32) + nn(ctx[...], wo[...]) + bo[...]).astype(BF16).astype(F32)
    xhat, rstd = standardize(resid)
    h2 = (xhat * gain[...] + bias[...]).astype(BF16)
    h2_out[...] = h2
    ready(1)
    ready(2)
    y_acc = jnp.zeros((L, D), F32)
    dh_acc = jnp.zeros((L, D), F32)
    for step in range(FF // cols):
        sl = slice(step * cols, (step + 1) * cols)
        pre_act = nn(h2, w1[:, sl]) + b1[:, sl]
        act, du = gelu_and_grad(pre_act, nt(dy[...], w2[sl, :]))
        col_sums[:, sl] += sum_groups(du)
        act, du = act.astype(BF16), du.astype(BF16)
        act_out[:, sl] = act
        du_out[:, sl] = du
        y_acc += nn(act, w2[sl, :])
        dh_acc += nt(du, w1[:, sl])
    y_out[...] = (resid + y_acc + b2[...]).astype(BF16)
    dy_f32 = dy[...].astype(F32)
    da = norm_input_grad(dh_acc, gain[...], xhat, rstd) + dy_f32
    da_out[...] = da
    da_b = da.astype(BF16)
    dab_out[...] = da_b
    dctx_out[...] = nt(da_b, wo[...]).astype(BF16)
    row_sums[0] += sum_groups(dh_acc * xhat)
    row_sums[1] += sum_groups(dh_acc)
    row_sums[2] += sum_groups(da)
    row_sums[3] += sum_groups(dy_f32)


def attn_bwd_body(ready, meta, lens, x, q, k, v, dctx, stats, da, gain, cos, sin, cos_t, sin_t, rows_in, q_in, kv_in, w, dx_out, dqkv_out, row_sums, q_sums, kv_sums, k_t, dq_t):
    @pl.when(pl.program_id(0) == 0)
    def _():
        row_sums[...] = rows_in[...]
        q_sums[...] = q_in[...]
        kv_sums[...] = kv_in[...]

    seq_len = lens[meta[0] + pl.program_id(0)]
    k_t[...] = k[...].T
    key_ok = lax.broadcasted_iota(jnp.int32, (L, L), 0) < seq_len
    half = HEAD // 2

    def products(head):
        lanes = pair_lanes(head)
        return nt(only_head(k[:, lanes], head), q[:, lanes]), nt(only_head(v[:, lanes], head), dctx[:, lanes])

    def softmax_grad(head, scores, d_probs):
        probs = jnp.exp(jnp.where(key_ok, scores, MASKED) - stats[0, head:head + 1, :]) * stats[0, HEADS + head:HEADS + head + 1, :]
        d_scores = probs * (d_probs - jnp.sum(d_probs * probs, axis=0, keepdims=True))
        return probs.astype(BF16), d_scores.astype(BF16)

    pending = {}

    def gradients(head, probs, d_scores):
        lanes = pair_lanes(head)
        dv = nn(probs, only_head(dctx[:, lanes], head))
        dk = nn(d_scores, only_head(q[:, lanes], head))
        dq = nn(k_t[head * HEAD:(head + 1) * HEAD, :], d_scores)
        low = (dq[:half] * cos_t[...] + dq[half:] * sin_t[...]) * HEAD ** -0.5
        high = (dq[half:] * cos_t[...] - dq[:half] * sin_t[...]) * HEAD ** -0.5
        for first, part in ((head * HEAD, low), (head * HEAD + half, high)):
            rows = slice(first, first + half)
            q_sums[rows, :] += part[:, :LANES] + part[:, LANES:]
            dq_t[rows, :] = part.astype(BF16)
        if head % 2 == 0:
            pending[head // 2] = dv, dk
            return
        dv_first, dk_first = pending.pop(head // 2)
        dv, dk = dv_first + dv, dk_first + dk
        dk = dk * cos[...] - swap_halves(dk) * sin[...]
        kv_sums[0, :, lanes] += sum_groups(dk)
        kv_sums[1, :, lanes] += sum_groups(dv)
        dqkv_out[:, pair_lanes(head, D)] = dk.astype(BF16)
        dqkv_out[:, pair_lanes(head, 2 * D)] = dv.astype(BF16)

    ahead = 2
    first = [products(head) for head in range(ahead)]
    second = None
    for head in range(HEADS):
        if head + ahead < HEADS:
            first.append(products(head + ahead))
        if second is not None:
            gradients(head - 1, *second)
        second = softmax_grad(head, *first[head])
        first[head] = None
    gradients(HEADS - 1, *second)
    dqkv_out[:, :D] = dq_t[...].T
    ready(0)
    dh = nt(dqkv_out[...], w[...])
    xhat, rstd = standardize(x[...].astype(F32))
    dx_out[...] = (da[...] + norm_input_grad(dh, gain[...], xhat, rstd)).astype(BF16)
    row_sums[0] += sum_groups(dh * xhat)
    row_sums[1] += sum_groups(dh)


def weight_grad_body(store, meta, lhs, rhs, *rest):
    partner, out = rest if len(rest) == 2 else (None, rest[0])
    acc = tn(lhs[...], rhs[...])
    k_step = pl.program_id(1)

    @pl.when(k_step == 0)
    def _():
        for at, part in store(acc):
            out[at] = part if partner is None else part + partner[at]

    @pl.when(k_step > 0)
    def _():
        for at, part in store(acc):
            out[at] += part


class Placing:
    def __init__(self, pieces, target, chunk):
        self.pieces, self.target, self.chunk = pieces, target, chunk

    def moves(self, steps):
        return 1 << (steps.bit_length() - 1)

    def rows_per_step(self, steps):
        return self.pieces[0].shape[0] // self.moves(steps)

    def scratch(self, steps):
        n = len(self.pieces)
        return [pltpu.VMEM((2, n, self.rows_per_step(steps), D), BF16), pltpu.SemaphoreType.DMA((2, n)), pltpu.SemaphoreType.DMA((2, n))]

    def hooks(self, steps, step, meta, pieces, target, buf, in_sem, out_sem):
        rows = self.rows_per_step(steps)
        total = self.pieces[0].shape[0]

        def fetch(j, s):
            return pltpu.make_async_copy(pieces[j].at[pl.ds(s * rows, rows)], buf.at[s % 2, j], in_sem.at[s % 2, j])

        def put(j, s):
            row = pl.multiple_of((meta[3] * TP + jnp.bitwise_xor(meta[1], j)) * total + s * rows, rows)
            return pltpu.make_async_copy(buf.at[s % 2, j], target.at[pl.ds(row, rows)], out_sem.at[s % 2, j])

        every = range(len(self.pieces))
        moves = self.moves(steps)

        def before():
            @pl.when((step >= 2) & (step < moves))
            def _():
                for j in every:
                    put(j, step - 2).wait()

            @pl.when(step < moves)
            def _():
                for j in every:
                    fetch(j, step).start()

        def after():
            @pl.when(step < moves)
            def _():
                for j in every:
                    fetch(j, step).wait()
                    put(j, step).start()

            @pl.when(step == moves - 1)
            def _():
                for j in every:
                    put(j, step - 1).wait()
                    put(j, step).wait()

        return before, after


def call(body, grid, scalars, streams, consts, weights, outs, prior, scratch, flops, n_bytes, placing=None, hand_on=False):
    steps = 1
    for size in grid:
        steps *= size

    def whole(array):
        return pl.BlockSpec(array.shape, lambda *_: (0,) * array.ndim, pipeline_mode=pl.Buffered(1))

    anywhere = pl.BlockSpec(memory_space=pl.ANY)
    n_scalar, n_stream, n_const, n_weight, n_out = len(scalars), len(streams), len(consts), len(weights), len(outs)
    operands = [a for a, _, _ in streams] + list(consts) + [a for a, _, _ in weights] + list(prior.values())
    in_specs = [pl.BlockSpec(block, index) for _, block, index in streams] + [whole(a) for a in consts] + [anywhere] * (n_weight + len(prior))
    aliases = {n_scalar + n_stream + n_const + n_weight + i: out for i, out in enumerate(prior)}
    out_specs = [pl.BlockSpec(block, index) for _, _, block, index in outs]
    out_shape = [jax.ShapeDtypeStruct(shape, dtype) for shape, dtype, _, _ in outs]
    n_hand = n_weight if hand_on else 0
    n_piece = 0
    scratches = [pltpu.VMEM(shape, BF16) for _, shape, _ in weights] + [pltpu.SemaphoreType.DMA((len(moves),)) for _, _, moves in weights]
    if placing is not None:
        n_piece = len(placing.pieces)
        aliases[n_scalar + len(operands) + n_piece] = n_out
        operands += list(placing.pieces) + [placing.target]
        in_specs += [anywhere] * (n_piece + 1)
        out_specs.append(anywhere)
        out_shape.append(jax.ShapeDtypeStruct(placing.target.shape, placing.target.dtype))
        scratches += placing.scratch(steps)
    out_specs += [anywhere] * n_hand
    out_shape += [jax.ShapeDtypeStruct(shape, BF16) for _, shape, _ in weights[:n_hand]]
    scratches += [pltpu.SemaphoreType.DMA((n_hand,))] * bool(n_hand) + scratch

    def kernel(*refs):
        refs = list(refs)

        def take(n):
            taken = refs[:n]
            del refs[:n]
            return taken

        scalar_refs, stream_refs, const_refs, weight_refs = take(n_scalar), take(n_stream), take(n_const), take(n_weight)
        take(len(prior))
        piece_refs = take(n_piece)
        if placing is not None:
            take(1)
        out_refs = take(n_out)
        target = take(1) if placing is not None else None
        handed = take(n_hand)
        held, sems = take(n_weight), take(n_weight)
        step = pl.program_id(0)
        for axis in range(1, len(grid)):
            step = step * grid[axis] + pl.program_id(axis)

        copies = [[pltpu.make_async_copy(ref.at[source] if source else ref, to.at[dest] if dest else to, sem.at[i]) for i, (source, dest) in enumerate(moves)]
                  for (_, _, moves), ref, to, sem in zip(weights, weight_refs, held, sems)]

        def ready(which):
            @pl.when(step == 0)
            def _():
                for copy in copies[which]:
                    copy.wait()

        if n_weight:
            @pl.when(step == 0)
            def _():
                for copy in sum(copies, []):
                    copy.start()

        if placing is not None:
            before, after = placing.hooks(steps, step, scalar_refs[0], piece_refs, target[0], *take(3))
            before()
        if n_hand:
            hand_sem, = take(1)
            hands = [pltpu.make_async_copy(ref, to, hand_sem.at[i]) for i, (ref, to) in enumerate(zip(held, handed))]

            @pl.when(step == 1)
            def _():
                for copy in hands:
                    copy.start()

        body(*([ready] if n_weight else []), *scalar_refs, *stream_refs, *const_refs, *held, *out_refs, *refs)
        if placing is not None:
            after()
        if n_hand:
            @pl.when(step == steps - 1)
            def _():
                for copy in hands:
                    copy.wait()

    return pl.pallas_call(
        kernel,
        grid_spec=pltpu.PrefetchScalarGridSpec(num_scalar_prefetch=n_scalar, grid=grid, in_specs=in_specs, out_specs=out_specs, scratch_shapes=scratches),
        out_shape=out_shape, input_output_aliases=aliases,
        compiler_params=pltpu.CompilerParams(dimension_semantics=("arbitrary",) * len(grid), vmem_limit_bytes=VMEM_LIMIT),
        cost_estimate=pl.CostEstimate(flops=flops, bytes_accessed=n_bytes, transcendentals=0))(*scalars, *operands)


def uninitialized(shape, dtype):
    return pl.pallas_call(lambda out: None, out_specs=pl.BlockSpec(memory_space=pl.ANY),
                          out_shape=jax.ShapeDtypeStruct(shape, dtype), name="uninitialized")()


def send_around(block):
    across = lax.ppermute(block, 'x', SWAP)
    beside = lax.ppermute(block, 'core', SWAP)
    diagonal = lax.ppermute(across, 'core', SWAP)
    return [block, beside, across, diagonal]


def block_moves(tp_dim, tp_size, fsdp_dim, fsdp_size):
    moves = []
    for t in range(TP):
        for f in range(FSDP):
            dest = [None, None]
            dest[tp_dim] = pl.ds(t * tp_size, tp_size)
            dest[fsdp_dim] = pl.ds(f * fsdp_size, fsdp_size)
            moves.append(((t * FSDP + f,), tuple(dest)))
    return moves


def device_layer(x_in, seq_lens, grad_out, *weight_shards):
    p = dict(zip(PARAM_NAMES, weight_shards))
    n_seq = x_in.shape[0]
    rows_all = n_seq * L
    tp_index = (lax.axis_index('x') * 2 + lax.axis_index('core')).astype(jnp.int32)
    x_rows = x_in.reshape(rows_all, D)
    dy_rows = grad_out.reshape(rows_all, D)
    rows_mine = rows_all // TP
    rows_chunk = rows_mine // CHUNKS
    rows_part = rows_all // CHUNKS
    seqs_chunk = rows_chunk // L

    vec_names = FSDP_VECTORS + BOTH_VECTORS
    gather = functools.partial(lax.all_gather, axis_name=BOTH, axis=0, tiled=False)
    vec_all = gather(jnp.concatenate([p[name] for name in vec_names])).reshape(TP, FSDP, -1)
    vec, place = {}, 0
    for name in vec_names:
        size = p[name].shape[0]
        part = vec_all[:, :, place:place + size]
        vec[name] = (part[0] if name in FSDP_VECTORS else part).reshape(1, -1).astype(F32)
        place += size
    qkv_blocks = gather(jnp.stack([p[name].reshape(D // 2, D // 4) for name in ('w_query', 'w_key', 'w_value')]))
    qkv_moves = [((owner[0], part), (dest[0], pl.ds(part * D + dest[1].start, D // 4)))
                 for owner, dest in block_moves(1, D // 4, 0, D // 2) for part in range(3)]
    w_qkv = qkv_blocks, (D, 3 * D), qkv_moves
    w_out = gather(p['w_out'].reshape(D // 4, D // 2)), (D, D), block_moves(0, D // 4, 1, D // 2)
    w_fc1 = gather(p['w_fc1']), (D, FF), block_moves(1, FF // 4, 0, D // 2)
    w_fc2 = gather(p['w_fc2']), (FF, D), block_moves(0, FF // 4, 1, D // 2)
    b_qkv = jnp.concatenate([vec['b_query'], vec['b_key'], vec['b_value']], axis=1)
    cos, sin, cos_t, sin_t = rope_tables()

    y_full = uninitialized((rows_all, D), BF16)
    dx_full = uninitialized((rows_all, D), BF16)

    def shared(i, meta, *_):
        return meta[0] + i, 0

    def local(i, *_):
        return i, 0

    def kept(i, meta, *_):
        return meta[2] + i, 0

    def seq3(i, *_):
        return i, 0, 0

    def keep(width):
        return (rows_mine, width), BF16, (L, width), kept

    def pass_on(width, dtype=BF16):
        return (rows_chunk, width), dtype, (L, width), local

    def total(*shape):
        return shape, F32, shape, lambda i, *_: (0,) * len(shape)

    prior_m = {3: uninitialized((rows_mine, D), BF16), 4: uninitialized((rows_mine, FF), BF16), 5: uninitialized((rows_mine, FF), BF16), 6: uninitialized((rows_mine, D), BF16)}
    prior_b = {1: uninitialized((rows_mine, 3 * D), BF16)}
    grid = (seqs_chunk,)
    mlp, bwd = [None] * CHUNKS, [None] * CHUNKS
    y_pieces, dx_pieces = [None] * CHUNKS, [None] * CHUNKS
    x_stream = (x_rows, (L, D), shared)

    def meta_of(c, placing=None, core=0):
        return jnp.stack([jnp.asarray(value, jnp.int32) for value in (
            c * (n_seq // CHUNKS) + tp_index * seqs_chunk, tp_index, c * seqs_chunk, placing.chunk if placing else 0, core)])

    def spread(i, meta, *_):
        return i // seqs_chunk * (n_seq // CHUNKS) + meta[0] + i % seqs_chunk

    whole_move = [(None, None)]
    h1, q, k, v, ctx, stats, w_qkv = call(
        functools.partial(attn_fwd_body, spread), (rows_mine // L,), [meta_of(0), seq_lens],
        [(x_rows, (L, D), lambda i, meta, *_: (spread(i, meta), 0))],
        [b_qkv, vec['ln1_gain'], vec['ln1_bias'], cos, sin], [w_qkv],
        [((rows_mine, D), BF16, (L, D), local)] * 5 + [((rows_mine // L, 2 * HEADS, L), F32, (1, 2 * HEADS, L), seq3)], {}, [],
        rows_mine * (6 * D * D + 64 * L * D), rows_mine * D * 12 + 6 * D * D, hand_on=True)

    arranged = []
    sums_m = [jnp.zeros(shape, F32) for shape in ((4, 8, D), (8, FF))]
    sums_b = [jnp.zeros(shape, F32) for shape in ((2, 8, D), (D, LANES), (2, 8, D))]

    def run_mlp(c, placing=None):
        out = call(
            mlp_body, grid, [meta_of(c, placing)],
            [x_stream, (ctx, (L, D), kept), (dy_rows, (L, D), shared)],
            [vec['b_out'], vec['ln2_gain'], vec['ln2_bias'], vec['b_fc1'], vec['b_fc2']] + sums_m, arranged or [w_out, w_fc1, w_fc2],
            [pass_on(D), pass_on(D, F32), pass_on(D), keep(D), keep(FF), keep(FF), keep(D), total(4, 8, D), total(8, FF)],
            prior_m, [], rows_chunk * (4 * D * D + 16 * D * FF), rows_chunk * (D * 20 + FF * 4) + 18 * D * D, placing, hand_on=not arranged)
        if not arranged:
            arranged.extend((array, array.shape, whole_move) for array in out[9:])
        prior_m.update({i: out[i] for i in prior_m})
        mlp[c] = out
        sums_m[:] = out[7:9]
        y_pieces[c] = send_around(out[0])
        return out[9:] if placing else ()

    def run_bwd(c, placing=None):
        saved = [(array, (L, D), kept) for array in (q, k, v)] + [(mlp[c][2], (L, D), local)]
        out = call(
            attn_bwd_body, grid, [meta_of(c, placing), seq_lens],
            [x_stream] + saved + [(stats, (1, 2 * HEADS, L), lambda i, meta, *_: (meta[2] + i, 0, 0)), (mlp[c][1], (L, D), local)],
            [vec['ln1_gain'], cos, sin, cos_t, sin_t] + sums_b, [(w_qkv, w_qkv.shape, whole_move)],
            [pass_on(D), keep(3 * D), total(2, 8, D), total(D, LANES), total(2, 8, D)], prior_b,
            [pltpu.VMEM((D, L), BF16), pltpu.VMEM((D, L), BF16)],
            rows_chunk * (6 * D * D + 160 * L * D), rows_chunk * D * 22 + 6 * D * D, placing)
        prior_b.update({1: out[1]})
        bwd[c] = out
        sums_b[:] = out[2:5]
        dx_pieces[c] = send_around(out[0])
        return out[5:]

    def weight_grad(lhs, rhs, lhs_index, rhs_index, n_out, size, block, out_index, store, placing=None, tile=rows_chunk):
        return call(
            functools.partial(weight_grad_body, store), (n_out, rows_mine // tile), [meta_of(0, placing)],
            [(lhs, (tile, D), lhs_index), (rhs, (tile, D), rhs_index)], [], [],
            [((2, FSDP, 2) + size, F32, block, out_index)], {}, [],
            2 * n_out * rows_mine * D * D, n_out * rows_mine * D * 4, placing)

    def swap_halves_along(axis, halves):
        index = lax.axis_index(axis)
        theirs = lax.ppermute(lax.dynamic_index_in_dim(halves, 1 - index, keepdims=False), axis, SWAP)
        return lax.dynamic_index_in_dim(halves, index, keepdims=False) + theirs

    def scatter(grad):
        size = grad.shape[3:]
        pair = lax.psum_scatter(grad.reshape(-1, size[-1]), ('core', 'fsdp'), scatter_dimension=0, tiled=True).reshape((2,) + size)
        return swap_halves_along('x', pair)

    def by_row(n, k, *_):
        return k, 0

    def by_row_and_part(n, k, *_):
        return k, n

    def by_chunk(n, k, meta):
        return k * TP + meta[1], 0

    half, quarter = D // 2, D // 4
    owners = [(t, f) for t in range(TP) for f in range(FSDP)]

    def store_fc2(acc):
        return [((0, f, 0), acc[:, f * half:(f + 1) * half]) for f in range(FSDP)]

    def store_fc1(acc):
        return [((0, f, 0), acc[f * half:(f + 1) * half]) for f in range(FSDP)]

    def store_qkv(acc):
        return [((t % 2, f, t // 2, 0), acc[f * half:(f + 1) * half, t * quarter:(t + 1) * quarter]) for t, f in owners]

    def store_out(acc):
        return [((t % 2, f, t // 2), acc[t * quarter:(t + 1) * quarter, f * half:(f + 1) * half]) for t, f in owners]

    def store_v(acc):
        return [((t % 2, t // 2, f), acc[f * half:(f + 1) * half, t * quarter:(t + 1) * quarter]) for t, f in owners]

    def owner_block(n, k, *_):
        return n % 2, 0, n // 2, 0, 0

    grads = {}
    last = CHUNKS - 1
    run_mlp(0)
    run_bwd(0)
    run_mlp(1)
    run_bwd(1)
    y_full, = run_mlp(2, Placing(y_pieces[0], y_full, 0))
    dx_full, = run_mlp(3, Placing(dx_pieces[0], dx_full, 0))
    h2, act, du, da_b = mlp[last][3:7]
    grads['w_fc1'] = scatter(weight_grad(h2, du, by_row, by_row_and_part, TP, (half, FF // 4), (1, FSDP, 1, half, FF // 4), owner_block, store_fc1,
                                               tile=2 * rows_chunk)[0])
    y_full, = run_bwd(2, Placing(y_pieces[1], y_full, 1))
    grad, dx_full = weight_grad(act, dy_rows, by_row_and_part, by_chunk, TP, (FF // 4, half), (1, FSDP, 1, FF // 4, half), owner_block, store_fc2,
                                Placing(dx_pieces[1], dx_full, 1))
    grads['w_fc2'] = scatter(grad)
    y_full, = run_bwd(3, Placing(y_pieces[2], y_full, 2))
    dqkv = bwd[last][1]
    grad, y_full = weight_grad(h1, dqkv, by_row, by_row_and_part, 2, (2, half, quarter), (2, FSDP, 2, 1, half, quarter),
                               lambda n, k, *_: (0, 0, 0, n, 0, 0), store_qkv, Placing(y_pieces[last], y_full, last))
    qk_grad = scatter(grad)
    grad, dx_full = weight_grad(ctx, da_b, by_row, by_row, 1, (quarter, half), (2, FSDP, 2, quarter, half), lambda n, k, *_: (0,) * 5, store_out,
                                Placing(dx_pieces[2], dx_full, 2))
    for axis in ('core', 'fsdp', 'x'):
        grad = swap_halves_along(axis, grad)
    grads['w_out'] = grad.reshape(p['w_out'].shape)
    v_grad, = weight_grad(h1, dqkv, by_row, lambda n, k, *_: (k, 2), 1, (half, quarter), (2, FSDP, 2, half, quarter), lambda n, k, *_: (0,) * 5, store_v,
                          tile=2 * rows_chunk)
    for axis in ('core', 'x', 'fsdp'):
        v_grad = swap_halves_along(axis, v_grad)
    for name, grad in zip(('w_query', 'w_key', 'w_value'), (qk_grad[0], qk_grad[1], v_grad)):
        grads[name] = grad.reshape(p[name].shape)
    placing = Placing(dx_pieces[last], dx_full, last)
    dx_full, = call(lambda meta: None, (8,), [meta_of(0, placing)], [], [], [], [], {}, [], 10 ** 9, rows_part * D * 4, placing)

    rows_b, q_sums, kv_sums = sums_b
    rows = jnp.concatenate([rows_b, sums_m[0], kv_sums]).sum(axis=1)
    flat = jnp.concatenate([rows.reshape(-1), q_sums.sum(axis=1), sums_m[1].sum(axis=0)])
    for axis in ('core', 'fsdp', 'x'):
        flat = flat + lax.ppermute(flat, axis, SWAP)
    n_rows = len(FSDP_VECTORS)
    fsdp_index = lax.axis_index('fsdp')
    owner = tp_index * FSDP + fsdp_index
    by_fsdp = lax.dynamic_index_in_dim(flat[:n_rows * D].reshape(n_rows, FSDP, -1), fsdp_index, axis=1, keepdims=False)
    by_owner = lax.dynamic_index_in_dim(flat[n_rows * D:(n_rows + 3) * D].reshape(3, TP * FSDP, -1), owner, axis=1, keepdims=False)
    by_owner_ff = lax.dynamic_index_in_dim(flat[(n_rows + 3) * D:].reshape(TP * FSDP, -1), owner, keepdims=False)
    for name, grad in zip(('ln1_gain', 'ln1_bias', 'ln2_gain', 'ln2_bias', 'b_out', 'b_fc2'), by_fsdp):
        grads[name] = grad
    grads.update(b_key=by_owner[0], b_value=by_owner[1], b_query=by_owner[2], b_fc1=by_owner_ff)
    return (y_full.reshape(x_in.shape), dx_full.reshape(x_in.shape)) + tuple(grads[name] for name in PARAM_NAMES)


def solution(mesh):
    split = jax.sharding.Mesh(mesh.devices.reshape(FSDP, 2, 2), ('fsdp', 'x', 'core'))
    act_spec = P('fsdp', None, None)
    weight_specs = tuple(PARAM_SPECS.values())
    return jax.shard_map(device_layer, mesh=split, in_specs=(act_spec, ROWS, act_spec) + weight_specs,
                         out_specs=(act_spec, act_spec) + weight_specs, check_vma=False)
```
